32 devices in a mesh: grp: 4 (over z), mem: 8 (over y, x, core).
Axes of the slice: x: 2, y: 2, z: 4, core: 2. Of those that a mesh axis runs over, the one named last changes fastest.
Arguments:
- embeddings: bfloat16 [32768, 4096], P(('grp', 'mem')), may hold values from -6 to 6
- local_picks: int32 [4, 64], P('grp', 'mem'), may hold values from 0 to 1023
- second_picks: int32 [4, 16], P('grp'), may hold values from 0 to 63
- final_picks: int32 [16], replicated, may hold values from 0 to 63
Outputs:
- gain_table: float32 [64, 64], P('grp', 'mem')
- final_cover: float32 [32768], P(('grp', 'mem'))
The draws below stay inside these ranges and needn't reach their ends.
Inputs may be any that keep to these rules, and one draw needn't show every extreme that they name: `local_picks`: entry (g, m * 8 + k) names a row among the 1024 points of device m of group g; repeats may occur. `second_picks`: candidate indices of the group, in greedy order; repeats may occur. `final_picks`: index g * 16 + t names group g's second-round pick t; repeats may occur.
All inputs are finite; a program needn't handle non-finite values.
Results may differ from the reference program's by a relative error of at most 0.0003.
Values may be sent and summed in bfloat16 or wider, within the bound.
A program may use at most 64 MiB of HBM per device.

```python
import jax
import jax.numpy as jnp
from jax import lax

D = 4096
P_DEV = 1024
K1 = 8
K2 = 16
K3 = 16
CANDS = 64
UNION = 64
POINTS = 32768
N_GRP = 4
N_MEM = 8


def plant(result, own_key, low, top_value):
    spot = [jax.random.randint(jax.random.fold_in(own_key, axis), (), 0, length) for axis, length in enumerate(result.shape)]
    widest = result.shape.index(max(result.shape))
    beside = spot[:widest] + [(spot[widest] + 1) % result.shape[widest]] + spot[widest + 1:]
    return result.at[tuple(spot)].set(low).at[tuple(beside)].set(top_value)


def steps_of(key, shape, pieces, low, largest):
    level, own = 1.0, jax.random.fold_in(key, 6)
    for position, blocks in pieces:
        heights = jnp.exp(jax.random.uniform(jax.random.fold_in(own, position), (blocks,), jnp.float32, low / len(pieces), largest / len(pieces)))
        level = level * jnp.repeat(heights, shape[position] // blocks).reshape([-1 if axis == position else 1 for axis in range(len(shape))])
    return level


def normal_values(stream_key, shape, spread, most, cuts=(), held_as=jnp.bfloat16):
    drawn = spread * jax.random.normal(stream_key, shape, jnp.float32)
    if cuts:
        drawn = drawn * steps_of(stream_key, shape, cuts, -0.22, 0.18)
    return jnp.clip(drawn, -most, most).astype(held_as)


def setup_inputs(seed: int = 0) -> dict:
    key_list = jax.random.split(jax.random.key(seed), 5)
    embeddings = normal_values(key_list[0], (POINTS, D), 1.0, 6.0, ((0, 32),))
    local_picks = plant(jax.random.randint(key_list[1], (N_GRP, CANDS), 0, P_DEV), jax.random.fold_in(key_list[1], 1), 0, P_DEV - 1).astype(jnp.int32)
    second_picks = plant(jax.random.randint(key_list[2], (N_GRP, K2), 0, CANDS), jax.random.fold_in(key_list[2], 1), 0, CANDS - 1).astype(jnp.int32)
    final_picks = plant(jax.random.randint(key_list[3], (K3,), 0, UNION), jax.random.fold_in(key_list[3], 1), 0, UNION - 1).astype(jnp.int32)
    return {"embeddings": embeddings, "local_picks": local_picks, "second_picks": second_picks, "final_picks": final_picks}


def reference(embeddings, local_picks, second_picks, final_picks):
    scaling = float(D) ** -0.5
    grouped = embeddings.reshape(N_GRP, N_MEM, P_DEV, D)
    pick_rows = local_picks.reshape(N_GRP, N_MEM, K1).astype(jnp.int32)
    candidates = jax.vmap(jax.vmap(lambda points, chosen: jnp.take(points, chosen, axis=0)))(grouped, pick_rows)
    candidates = candidates.reshape(N_GRP, CANDS, D)
    winners = jax.vmap(lambda cands, chosen: jnp.take(cands, chosen, axis=0))(candidates, second_picks.astype(jnp.int32))
    winners = winners.reshape(UNION, D)
    final_rows = jnp.take(winners, final_picks.astype(jnp.int32), axis=0)

    def group_gains(inputs):
        cand_group, points_group, second_group = inputs

        def device_step(running, device_inputs):
            point_rows, member = device_inputs
            similar_map = jnp.dot(point_rows, cand_group.T, preferred_element_type=jnp.float32) * scaling
            own_block = lax.dynamic_slice_in_dim(similar_map, member * K1, K1, 1)
            coverage = jnp.max(own_block, axis=1)
            chosen_cols = jnp.take(similar_map, second_group, axis=1)

            def greedy_step(cover_now, column):
                partial_value = jnp.sum(jnp.maximum(similar_map - cover_now[:, None], 0.0), axis=0)
                return jnp.maximum(cover_now, column), partial_value

            _, partials = lax.scan(greedy_step, coverage, chosen_cols.T)
            return running + partials, None

        start_sum = jnp.zeros((K2, CANDS), jnp.float32)
        running, _ = lax.scan(device_step, start_sum, (points_group, jnp.arange(N_MEM, dtype=jnp.int32)))
        return running / P_DEV

    gain_table = lax.map(group_gains, (candidates, grouped, second_picks.astype(jnp.int32)))
    gain_table = gain_table.reshape(N_GRP * K2, CANDS)

    def device_cover(point_rows):
        return jnp.max(jnp.dot(point_rows, final_rows.T, preferred_element_type=jnp.float32) * scaling, axis=1)

    final_cover = lax.map(device_cover, embeddings.reshape(N_GRP * N_MEM, P_DEV, D)).reshape(POINTS)
    return gain_table, final_cover
```

```python
import functools

import jax
import jax.numpy as jnp
from jax import lax
from jax.experimental import pallas as pl
from jax.experimental.pallas import tpu as pltpu
from jax.sharding import PartitionSpec as P

MESH = pl.DeviceIdType.MESH
NT = (((1,), (1,)), ((), ()))
LOADS = 8
BLOCK = 16


def kernel(
    n_grp, n_mem, slices,
    emb_hbm, local_hbm, second_hbm, final_hbm,
    gain_ref, cover_ref,
    emb, local, second, final, own, part, cand, zbuf, zsum, fin, sim, gsend, gbuf,
    load_sem, pick_sem, part_send, part_recv, cand_send, cand_recv,
    z_send, z_recv, fin_send, fin_recv, g_send, g_recv,
):
    grp = lax.axis_index("grp")
    mem = lax.axis_index("mem")
    tiles, block, depth = emb.shape
    points = tiles * block
    k1 = own.shape[0]
    k2 = second.shape[1]
    k3 = final.shape[0]
    cands = n_mem * k1
    width = depth // slices
    scale = float(depth) ** -0.5
    every = slices == n_mem

    def owner(body):
        if every:
            body()
        else:
            pl.when(mem < slices)(body)

    def mem_peer(d):
        return lax.rem(mem + d, n_mem)

    def grp_peer(d):
        return lax.rem(grp + d, n_grp)

    barrier = pltpu.get_barrier_semaphore()
    for d in range(1, n_mem):
        pl.semaphore_signal(barrier, inc=1, device_id={"mem": mem_peer(d)}, device_id_type=MESH)
    for d in range(1, n_grp):
        pl.semaphore_signal(barrier, inc=1, device_id={"grp": grp_peer(d)}, device_id_type=MESH)

    picks = [
        pltpu.make_async_copy(src, dst, pick_sem.at[i])
        for i, (src, dst) in enumerate(((local_hbm, local), (second_hbm, second), (final_hbm, final)))
    ]
    for copy in picks:
        copy.start()
    rows = tiles // LOADS
    loads = [
        pltpu.make_async_copy(
            emb_hbm.at[pl.ds(i * rows, rows)], emb.at[pl.ds(i * rows, rows)], load_sem.at[i]
        )
        for i in range(LOADS)
    ]
    for copy in loads:
        copy.start()
    for copy in picks:
        copy.wait()

    def one_hot(values, lanes):
        line = lax.broadcasted_iota(jnp.int32, (len(values), lanes), 0)
        spot = lax.broadcasted_iota(jnp.int32, (len(values), lanes), 1)
        wanted = jnp.zeros((len(values), lanes), jnp.int32)
        for r, value in enumerate(values):
            wanted = jnp.where(line == r, value, wanted)
        return jnp.where(spot == wanted, 1.0, 0.0).astype(jnp.bfloat16)

    shift = block.bit_length() - 1
    starts = [local[0, r] >> shift for r in range(k1)]
    choose = one_hot([r * block + (local[0, r] & (block - 1)) for r in range(k1)], k1 * block)
    seconds = one_hot([second[0, t] for t in range(k2)], cands)
    finals_of = one_hot([final[j] - grp * k2 for j in range(k3)], k2)
    table = jnp.dot(finals_of, seconds, preferred_element_type=jnp.float32).astype(jnp.bfloat16)

    for copy in loads:
        copy.wait()
    step = depth // 4
    for c in range(0, depth, step):
        blocks = jnp.concatenate(
            [emb[s, :, c:c + step] for s in starts], axis=0
        )
        own[:, c:c + step] = jnp.dot(
            choose, blocks, preferred_element_type=jnp.float32
        ).astype(jnp.bfloat16)
    pl.semaphore_wait(barrier, n_mem - 1 + n_grp - 1)

    def part_copy(d):
        peer = mem_peer(d)
        return pltpu.make_async_remote_copy(
            src_ref=own.at[:, pl.ds(pl.multiple_of(lax.rem(peer, slices) * width, 128), width)],
            dst_ref=part.at[mem],
            send_sem=part_send.at[d - 1],
            recv_sem=part_recv.at[d - 1],
            device_id={"mem": peer},
            device_id_type=MESH,
        )

    parts = [part_copy(d) for d in range(1, n_mem)]
    for copy in parts:
        copy.start()
    bulks = [
        pltpu.make_async_remote_copy(
            src_ref=own,
            dst_ref=cand.at[mem],
            send_sem=cand_send.at[d - 1],
            recv_sem=cand_recv.at[d - 1],
            device_id={"mem": mem_peer(d)},
            device_id_type=MESH,
        )
        for d in range(1, n_mem)
    ]
    for copy in bulks:
        copy.start()
    my_cols = pl.ds(pl.multiple_of(lax.rem(mem, slices) * width, 128), width)
    part[mem] = own[:, my_cols]
    cand[mem] = own[...]

    for copy in parts:
        copy.wait_recv()
    share = jnp.dot(
        table, part[...].reshape(cands, width), preferred_element_type=jnp.float32
    ).astype(jnp.bfloat16)
    zbuf[grp] = share
    shares = [
        pltpu.make_async_remote_copy(
            src_ref=zbuf.at[grp],
            dst_ref=zbuf.at[grp],
            send_sem=z_send.at[d - 1],
            recv_sem=z_recv.at[d - 1],
            device_id={"grp": grp_peer(d)},
            device_id_type=MESH,
        )
        for d in range(1, n_grp)
    ]
    for copy in shares:
        copy.start()

    for copy in bulks:
        copy.wait_recv()
    every_cand = cand[...].reshape(cands, depth)
    winners = jnp.dot(seconds, every_cand, preferred_element_type=jnp.float32).astype(jnp.bfloat16)
    rhs = jnp.concatenate([every_cand, winners], axis=0)
    tile = points // 4
    part_rows = tiles // 4

    def rows_of(i):
        return emb[i * part_rows:(i + 1) * part_rows].reshape(tile, depth)

    def similar(i):
        sim[:, i * tile:(i + 1) * tile] = lax.dot_general(
            rhs, rows_of(i), NT, preferred_element_type=jnp.float32
        )

    similar(0)
    similar(1)

    for copy in shares:
        copy.wait_recv()
    total = zbuf[0].astype(jnp.float32)
    for g in range(1, n_grp):
        total = total + zbuf[g].astype(jnp.float32)
    zsum[...] = total.astype(jnp.bfloat16)
    finals = [
        pltpu.make_async_remote_copy(
            src_ref=zsum,
            dst_ref=fin.at[:, my_cols],
            send_sem=fin_send.at[d - 1],
            recv_sem=fin_recv.at[d - 1],
            device_id={"mem": mem_peer(d)},
            device_id_type=MESH,
        )
        for d in range(1, n_mem)
    ]

    def send_final():
        for copy in finals:
            copy.start()
        fin[:, my_cols] = zsum[...]

    owner(send_final)

    similar(2)
    similar(3)

    cover = jnp.max(sim[pl.ds(pl.multiple_of(mem * k1, k1), k1), :], axis=0, keepdims=True)
    lane = lax.broadcasted_iota(jnp.int32, (cands, 128), 1)
    gains = jnp.zeros((cands, 128), jnp.float32)
    for t in range(k2):
        acc = jnp.zeros((cands, 128), jnp.float32)
        for c in range(0, points, 128):
            acc = acc + jnp.maximum(sim[:cands, c:c + 128] - cover[:, c:c + 128], 0.0)
        gains = jnp.where(lane == t, jnp.sum(acc, axis=1, keepdims=True), gains)
        cover = jnp.maximum(cover, sim[cands + t:cands + t + 1, :])
    gsend[...] = gains.reshape(n_mem, k1, 128)
    gathers = [
        pltpu.make_async_remote_copy(
            src_ref=gsend.at[mem_peer(d)],
            dst_ref=gbuf.at[mem],
            send_sem=g_send.at[d - 1],
            recv_sem=g_recv.at[d - 1],
            device_id={"mem": mem_peer(d)},
            device_id_type=MESH,
        )
        for d in range(1, n_mem)
    ]
    for copy in gathers:
        copy.start()
    gbuf[mem] = gsend[mem]

    if every:
        for copy in finals:
            copy.wait_recv()
    else:
        for d in range(1, n_mem):
            pl.when(lax.rem(mem + n_mem - d, n_mem) < slices)(finals[d - 1].wait_recv)
    final_rows = fin[...]
    for i in range(4):
        best = lax.dot_general(
            final_rows, rows_of(i), NT, preferred_element_type=jnp.float32
        )
        cover_ref[:, i * tile:(i + 1) * tile] = jnp.max(best, axis=0, keepdims=True) * scale

    for copy in gathers:
        copy.wait_recv()
    total = jnp.sum(gbuf[...], axis=0) * (scale / points)
    wide = jnp.concatenate([total, jnp.zeros((128 - k1, 128), jnp.float32)], axis=0)
    gain_ref[...] = wide.T[:k2, :k1]

    for copy in parts + bulks + shares + gathers:
        copy.wait_send()

    def sent_final():
        for copy in finals:
            copy.wait_send()

    owner(sent_final)


def per_device(n_grp, n_mem, embeddings, local_picks, second_picks, final_picks):
    points, depth = embeddings.shape
    k1 = local_picks.shape[1]
    k2 = second_picks.shape[1]
    k3 = final_picks.shape[0]
    cands = n_mem * k1
    slices = min(n_mem, depth // 128)
    width = depth // slices
    half = jnp.bfloat16
    dma = pltpu.SemaphoreType.DMA
    gain, cover = pl.pallas_call(
        functools.partial(kernel, n_grp, n_mem, slices),
        out_shape=(
            jax.ShapeDtypeStruct((k2, k1), jnp.float32),
            jax.ShapeDtypeStruct((1, points), jnp.float32),
        ),
        in_specs=[pl.BlockSpec(memory_space=pl.ANY)] * 4,
        out_specs=(pl.BlockSpec(memory_space=pltpu.VMEM),) * 2,
        scratch_shapes=[
            pltpu.VMEM((points // BLOCK, BLOCK, depth), half),
            pltpu.SMEM(local_picks.shape, jnp.int32),
            pltpu.SMEM(second_picks.shape, jnp.int32),
            pltpu.SMEM(final_picks.shape, jnp.int32),
            pltpu.VMEM((k1, depth), half),
            pltpu.VMEM((n_mem, k1, width), half),
            pltpu.VMEM((n_mem, k1, depth), half),
            pltpu.VMEM((n_grp, k3, width), half),
            pltpu.VMEM((k3, width), half),
            pltpu.VMEM((k3, depth), half),
            pltpu.VMEM((cands + k2, points), jnp.float32),
            pltpu.VMEM((n_mem, k1, 128), jnp.float32),
            pltpu.VMEM((n_mem, k1, 128), jnp.float32),
            dma((LOADS,)), dma((3,)),
            dma((n_mem - 1,)), dma((n_mem - 1,)),
            dma((n_mem - 1,)), dma((n_mem - 1,)),
            dma((n_grp - 1,)), dma((n_grp - 1,)),
            dma((n_mem - 1,)), dma((n_mem - 1,)),
            dma((n_mem - 1,)), dma((n_mem - 1,)),
        ],
        compiler_params=pltpu.CompilerParams(
            collective_id=0, has_side_effects=True, vmem_limit_bytes=48 * 1024 * 1024
        ),
    )(embeddings.reshape(points // BLOCK, BLOCK, depth), local_picks, second_picks, final_picks)
    return gain, cover.reshape(points)


def solution(mesh):
    n_grp, n_mem = mesh.shape["grp"], mesh.shape["mem"]
    return jax.shard_map(
        functools.partial(per_device, n_grp, n_mem),
        mesh=mesh,
        in_specs=(P(("grp", "mem"), None), P("grp", "mem"), P("grp", None), P()),
        out_specs=(P("grp", "mem"), P(("grp", "mem"))),
        check_vma=False,
    )
```

```python
import functools

import jax
import jax.numpy as jnp
from jax import lax
from jax.experimental import pallas as pl
from jax.experimental.pallas import tpu as pltpu
from jax.sharding import PartitionSpec as P

MESH = pl.DeviceIdType.MESH
NT = (((1,), (1,)), ((), ()))
LOADS = 8
BLOCK = 16


def kernel(
    n_grp, n_mem, slices,
    emb_hbm, local_hbm, second_hbm, final_hbm,
    gain_ref, cover_ref,
    emb, local, second, final, own, part, cand, zbuf, zsum, fin, sim, gsend, gbuf,
    load_sem, pick_sem, part_send, part_recv, cand_send, cand_recv,
    z_send, z_recv, fin_send, fin_recv, g_send, g_recv,
):
    grp = lax.axis_index("grp")
    mem = lax.axis_index("mem")
    tiles, block, depth = emb.shape
    points = tiles * block
    k1 = own.shape[0]
    k2 = second.shape[1]
    k3 = final.shape[0]
    cands = n_mem * k1
    width = depth // slices
    scale = float(depth) ** -0.5
    every = slices == n_mem

    def owner(body):
        if every:
            body()
        else:
            pl.when(mem < slices)(body)

    def mem_peer(d):
        return lax.rem(mem + d, n_mem)

    def grp_peer(d):
        return lax.rem(grp + d, n_grp)

    barrier = pltpu.get_barrier_semaphore()
    for d in range(1, n_mem):
        pl.semaphore_signal(barrier, inc=1, device_id={"mem": mem_peer(d)}, device_id_type=MESH)
    for d in range(1, n_grp):
        pl.semaphore_signal(barrier, inc=1, device_id={"grp": grp_peer(d)}, device_id_type=MESH)

    picks = [
        pltpu.make_async_copy(src, dst, pick_sem.at[i])
        for i, (src, dst) in enumerate(((local_hbm, local), (second_hbm, second), (final_hbm, final)))
    ]
    for copy in picks:
        copy.start()
    rows = tiles // LOADS
    loads = [
        pltpu.make_async_copy(
            emb_hbm.at[pl.ds(i * rows, rows)], emb.at[pl.ds(i * rows, rows)], load_sem.at[i]
        )
        for i in range(LOADS)
    ]
    for copy in loads:
        copy.start()
    for copy in picks:
        copy.wait()

    def one_hot(values, lanes):
        line = lax.broadcasted_iota(jnp.int32, (len(values), lanes), 0)
        spot = lax.broadcasted_iota(jnp.int32, (len(values), lanes), 1)
        wanted = jnp.zeros((len(values), lanes), jnp.int32)
        for r, value in enumerate(values):
            wanted = jnp.where(line == r, value, wanted)
        return jnp.where(spot == wanted, 1.0, 0.0).astype(jnp.bfloat16)

    shift = block.bit_length() - 1
    starts = [local[0, r] >> shift for r in range(k1)]
    choose = one_hot([r * block + (local[0, r] & (block - 1)) for r in range(k1)], k1 * block)
    seconds = one_hot([second[0, t] for t in range(k2)], cands)
    finals_of = one_hot([final[j] - grp * k2 for j in range(k3)], k2)
    table = jnp.dot(finals_of, seconds, preferred_element_type=jnp.float32).astype(jnp.bfloat16)

    for copy in loads:
        copy.wait()
    step = depth // 4
    for c in range(0, depth, step):
        blocks = jnp.concatenate(
            [emb[s, :, c:c + step] for s in starts], axis=0
        )
        own[:, c:c + step] = jnp.dot(
            choose, blocks, preferred_element_type=jnp.float32
        ).astype(jnp.bfloat16)
    pl.semaphore_wait(barrier, n_mem - 1 + n_grp - 1)

    def part_copy(d):
        peer = mem_peer(d)
        return pltpu.make_async_remote_copy(
            src_ref=own.at[:, pl.ds(pl.multiple_of(lax.rem(peer, slices) * width, 128), width)],
            dst_ref=part.at[mem],
            send_sem=part_send.at[d - 1],
            recv_sem=part_recv.at[d - 1],
            device_id={"mem": peer},
            device_id_type=MESH,
        )

    parts = [part_copy(d) for d in range(1, n_mem)]
    for copy in parts:
        copy.start()
    bulks = [
        pltpu.make_async_remote_copy(
            src_ref=own,
            dst_ref=cand.at[mem],
            send_sem=cand_send.at[d - 1],
            recv_sem=cand_recv.at[d - 1],
            device_id={"mem": mem_peer(d)},
            device_id_type=MESH,
        )
        for d in range(1, n_mem)
    ]
    for copy in bulks:
        copy.start()
    my_cols = pl.ds(pl.multiple_of(lax.rem(mem, slices) * width, 128), width)
    part[mem] = own[:, my_cols]
    cand[mem] = own[...]

    for copy in parts:
        copy.wait_recv()
    share = jnp.dot(
        table, part[...].reshape(cands, width), preferred_element_type=jnp.float32
    ).astype(jnp.bfloat16)
    zbuf[grp] = share
    shares = [
        pltpu.make_async_remote_copy(
            src_ref=zbuf.at[grp],
            dst_ref=zbuf.at[grp],
            send_sem=z_send.at[d - 1],
            recv_sem=z_recv.at[d - 1],
            device_id={"grp": grp_peer(d)},
            device_id_type=MESH,
        )
        for d in range(1, n_grp)
    ]
    for copy in shares:
        copy.start()

    for copy in bulks:
        copy.wait_recv()
    every_cand = cand[...].reshape(cands, depth)
    winners = jnp.dot(seconds, every_cand, preferred_element_type=jnp.float32).astype(jnp.bfloat16)
    rhs = jnp.concatenate([every_cand, winners], axis=0)
    tile = points // 4
    part_rows = tiles // 4

    def rows_of(i):
        return emb[i * part_rows:(i + 1) * part_rows].reshape(tile, depth)

    def similar(i):
        sim[:, i * tile:(i + 1) * tile] = lax.dot_general(
            rhs, rows_of(i), NT, preferred_element_type=jnp.float32
        )

    similar(0)
    similar(1)

    for copy in shares:
        copy.wait_recv()
    total = zbuf[0].astype(jnp.float32)
    for g in range(1, n_grp):
        total = total + zbuf[g].astype(jnp.float32)
    zsum[...] = total.astype(jnp.bfloat16)
    finals = [
        pltpu.make_async_remote_copy(
            src_ref=zsum,
            dst_ref=fin.at[:, my_cols],
            send_sem=fin_send.at[d - 1],
            recv_sem=fin_recv.at[d - 1],
            device_id={"mem": mem_peer(d)},
            device_id_type=MESH,
        )
        for d in range(1, n_mem)
    ]

    def send_final():
        for copy in finals:
            copy.start()
        fin[:, my_cols] = zsum[...]

    owner(send_final)

    similar(2)
    similar(3)

    cover = jnp.max(sim[pl.ds(pl.multiple_of(mem * k1, k1), k1), :], axis=0, keepdims=True)
    lane = lax.broadcasted_iota(jnp.int32, (cands, 128), 1)
    gains = jnp.zeros((cands, 128), jnp.float32)
    for t in range(k2):
        acc = jnp.zeros((cands, 128), jnp.float32)
        for c in range(0, points, 128):
            acc = acc + jnp.maximum(sim[:cands, c:c + 128] - cover[:, c:c + 128], 0.0)
        gains = jnp.where(lane == t, jnp.sum(acc, axis=1, keepdims=True), gains)
        cover = jnp.maximum(cover, sim[cands + t:cands + t + 1, :])
    gsend[...] = gains.reshape(n_mem, k1, 128)
    gathers = [
        pltpu.make_async_remote_copy(
            src_ref=gsend.at[mem_peer(d)],
            dst_ref=gbuf.at[mem],
            send_sem=g_send.at[d - 1],
            recv_sem=g_recv.at[d - 1],
            device_id={"mem": mem_peer(d)},
            device_id_type=MESH,
        )
        for d in range(1, n_mem)
    ]
    for copy in gathers:
        copy.start()
    gbuf[mem] = gsend[mem]

    if every:
        for copy in finals:
            copy.wait_recv()
    else:
        for d in range(1, n_mem):
            pl.when(lax.rem(mem + n_mem - d, n_mem) < slices)(finals[d - 1].wait_recv)
    final_rows = fin[...]
    for i in range(4):
        best = lax.dot_general(
            final_rows, rows_of(i), NT, preferred_element_type=jnp.float32
        )
        cover_ref[:, i * tile:(i + 1) * tile] = jnp.max(best, axis=0, keepdims=True) * scale

    for copy in gathers:
        copy.wait_recv()
    total = jnp.sum(gbuf[...], axis=0) * (scale / points)
    gain_ref[...] = total[:, :k2]

    for copy in parts + bulks + shares + gathers:
        copy.wait_send()

    def sent_final():
        for copy in finals:
            copy.wait_send()

    owner(sent_final)


def per_device(n_grp, n_mem, embeddings, local_picks, second_picks, final_picks):
    points, depth = embeddings.shape
    k1 = local_picks.shape[1]
    k2 = second_picks.shape[1]
    k3 = final_picks.shape[0]
    cands = n_mem * k1
    slices = min(n_mem, depth // 128)
    width = depth // slices
    half = jnp.bfloat16
    dma = pltpu.SemaphoreType.DMA
    gain, cover = pl.pallas_call(
        functools.partial(kernel, n_grp, n_mem, slices),
        out_shape=(
            jax.ShapeDtypeStruct((k1, k2), jnp.float32),
            jax.ShapeDtypeStruct((1, points), jnp.float32),
        ),
        in_specs=[pl.BlockSpec(memory_space=pltpu.HBM)] * 4,
        out_specs=(pl.BlockSpec(memory_space=pltpu.VMEM),) * 2,
        scratch_shapes=[
            pltpu.VMEM((points // BLOCK, BLOCK, depth), half),
            pltpu.SMEM(local_picks.shape, jnp.int32),
            pltpu.SMEM(second_picks.shape, jnp.int32),
            pltpu.SMEM(final_picks.shape, jnp.int32),
            pltpu.VMEM((k1, depth), half),
            pltpu.VMEM((n_mem, k1, width), half),
            pltpu.VMEM((n_mem, k1, depth), half),
            pltpu.VMEM((n_grp, k3, width), half),
            pltpu.VMEM((k3, width), half),
            pltpu.VMEM((k3, depth), half),
            pltpu.VMEM((cands + k2, points), jnp.float32),
            pltpu.VMEM((n_mem, k1, 128), jnp.float32),
            pltpu.VMEM((n_mem, k1, 128), jnp.float32),
            dma((LOADS,)), dma((3,)),
            dma((n_mem - 1,)), dma((n_mem - 1,)),
            dma((n_mem - 1,)), dma((n_mem - 1,)),
            dma((n_grp - 1,)), dma((n_grp - 1,)),
            dma((n_mem - 1,)), dma((n_mem - 1,)),
            dma((n_mem - 1,)), dma((n_mem - 1,)),
        ],
        compiler_params=pltpu.CompilerParams(
            collective_id=0, has_side_effects=True, vmem_limit_bytes=48 * 1024 * 1024
        ),
    )(embeddings.reshape(points // BLOCK, BLOCK, depth),
      *[pltpu.with_memory_space_constraint(x, pltpu.HBM) for x in (local_picks, second_picks, final_picks)])
    return gain.T, cover.reshape(points)


def solution(mesh):
    n_grp, n_mem = mesh.shape["grp"], mesh.shape["mem"]
    return jax.shard_map(
        functools.partial(per_device, n_grp, n_mem),
        mesh=mesh,
        in_specs=(P(("grp", "mem"), None), P("grp", "mem"), P("grp", None), P()),
        out_specs=(P("grp", "mem"), P(("grp", "mem"))),
        check_vma=False,
    )
```

```python
import functools

import jax
import jax.numpy as jnp
from jax import lax
from jax.experimental import pallas as pl
from jax.experimental.pallas import tpu as pltpu
from jax.sharding import PartitionSpec as P

MESH = pl.DeviceIdType.MESH
NT = (((1,), (1,)), ((), ()))
LOADS = 8
BLOCK = 16
PIECES = 2


def kernel(
    n_grp, n_mem, slices,
    emb_hbm, local_hbm, second_hbm, final_hbm,
    gain_ref, cover_ref,
    emb, local, second, final, own, part, cand, zbuf, zsum, fin, sim, gsend, gbuf,
    load_sem, pick_sem, part_send, part_recv, cand_send, cand_recv,
    z_send, z_recv, fin_send, fin_recv, g_send, g_recv,
):
    grp = lax.axis_index("grp")
    mem = lax.axis_index("mem")
    tiles, block, depth = emb.shape
    points = tiles * block
    k1 = own.shape[0]
    k2 = second.shape[1]
    k3 = final.shape[0]
    cands = n_mem * k1
    width = depth // slices
    scale = float(depth) ** -0.5
    every = slices == n_mem

    def owner(body):
        if every:
            body()
        else:
            pl.when(mem < slices)(body)

    def peer_of(own_place, count, d):
        peer = own_place
        for bit in (1 << k for k in range(count.bit_length() - 1)):
            if d & bit:
                peer = peer + bit - 2 * bit * ((own_place // bit) % 2)
        return peer

    mem_far = range(n_mem - 1, 0, -1)
    mem_near = range(1, n_mem)
    across = range(2, n_mem, 2)
    grp_far = range(n_grp - 1, 0, -1)
    mem_peers = {d: peer_of(mem, n_mem, d) for d in mem_far}
    grp_peers = {d: peer_of(grp, n_grp, d) for d in grp_far}

    barrier = pltpu.get_barrier_semaphore()
    for d in mem_far:
        pl.semaphore_signal(barrier, inc=1, device_id={"mem": mem_peers[d]}, device_id_type=MESH)
    for d in grp_far:
        pl.semaphore_signal(barrier, inc=1, device_id={"grp": grp_peers[d]}, device_id_type=MESH)

    picks = [
        pltpu.make_async_copy(src, dst, pick_sem.at[i])
        for i, (src, dst) in enumerate(((local_hbm, local), (second_hbm, second), (final_hbm, final)))
    ]
    for copy in picks:
        copy.start()
    rows = tiles // LOADS
    loads = [
        pltpu.make_async_copy(
            emb_hbm.at[pl.ds(i * rows, rows)], emb.at[pl.ds(i * rows, rows)], load_sem.at[i]
        )
        for i in range(LOADS)
    ]
    for copy in loads:
        copy.start()
    for copy in picks:
        copy.wait()

    def one_hot(values, lanes):
        line = lax.broadcasted_iota(jnp.int32, (len(values), lanes), 0)
        spot = lax.broadcasted_iota(jnp.int32, (len(values), lanes), 1)
        wanted = jnp.zeros((len(values), lanes), jnp.int32)
        for r, value in enumerate(values):
            wanted = jnp.where(line == r, value, wanted)
        return jnp.where(spot == wanted, 1.0, 0.0).astype(jnp.bfloat16)

    shift = block.bit_length() - 1
    starts = [local[0, r] >> shift for r in range(k1)]
    choose = one_hot([r * block + (local[0, r] & (block - 1)) for r in range(k1)], k1 * block)
    seconds = one_hot([second[0, t] for t in range(k2)], cands)
    finals_of = one_hot([final[j] - grp * k2 for j in range(k3)], k2)
    table = jnp.dot(finals_of, seconds, preferred_element_type=jnp.float32).astype(jnp.bfloat16)

    for copy in loads:
        copy.wait()
    step = depth // 4
    for c in range(0, depth, step):
        blocks = jnp.concatenate(
            [emb[s, :, c:c + step] for s in starts], axis=0
        )
        own[:, c:c + step] = jnp.dot(
            choose, blocks, preferred_element_type=jnp.float32
        ).astype(jnp.bfloat16)
    pl.semaphore_wait(barrier, n_mem - 1 + n_grp - 1)

    def part_copy(d):
        peer = mem_peers[d]
        return pltpu.make_async_remote_copy(
            src_ref=own.at[:, pl.ds(pl.multiple_of(lax.rem(peer, slices) * width, 128), width)],
            dst_ref=part.at[mem],
            send_sem=part_send.at[d - 1],
            recv_sem=part_recv.at[d - 1],
            device_id={"mem": peer},
            device_id_type=MESH,
        )

    parts = [part_copy(d) for d in mem_near]
    for copy in parts:
        copy.start()
    chunks, piece = cand.shape[0], cand.shape[3]

    chunks, piece = cand.shape[0], cand.shape[3]

    def bulk_copy(c, d, source, at, to):
        return pltpu.make_async_remote_copy(
            src_ref=source,
            dst_ref=cand.at[c, at],
            send_sem=cand_send.at[c, d - 1],
            recv_sem=cand_recv.at[c, d - 1],
            device_id={"mem": to},
            device_id_type=MESH,
        )

    bulks, relays = [], []
    for c in range(chunks):
        mine = own.at[:, c * piece:(c + 1) * piece]
        bulks.append([bulk_copy(c, d, mine, mem, mem_peers[d]) for d in across])
        relays.append([bulk_copy(c, 1, mine, mem, mem_peers[1])] + [
            bulk_copy(c, d + 1, cand.at[c, mem_peers[d]], mem_peers[d], mem_peers[1])
            for d in across
        ])
    for chunk in bulks:
        for copy in chunk:
            copy.start()
    for chunk in relays:
        chunk[0].start()
    my_cols = pl.ds(pl.multiple_of(lax.rem(mem, slices) * width, 128), width)
    part[mem] = own[:, my_cols]
    for c in range(chunks):
        cand[c, mem] = own[:, c * piece:(c + 1) * piece]

    for copy in parts:
        copy.wait_recv()
    share = jnp.dot(
        table, part[...].reshape(cands, width), preferred_element_type=jnp.float32
    ).astype(jnp.bfloat16)
    zbuf[grp] = share
    shares = [
        pltpu.make_async_remote_copy(
            src_ref=zbuf.at[grp],
            dst_ref=zbuf.at[grp],
            send_sem=z_send.at[d - 1],
            recv_sem=z_recv.at[d - 1],
            device_id={"grp": grp_peers[d]},
            device_id_type=MESH,
        )
        for d in grp_far
    ]
    for copy in shares:
        copy.start()

    def relay(c):
        for copy, onward in zip(bulks[c], relays[c][1:]):
            copy.wait_recv()
            onward.start()

    relay(0)
    for c in range(chunks):
        if c + 1 < chunks:
            relay(c + 1)
        for copy in relays[c]:
            copy.wait_recv()
        every_cand = cand[c].reshape(cands, piece)
        winners = jnp.dot(
            seconds, every_cand, preferred_element_type=jnp.float32
        ).astype(jnp.bfloat16)
        rhs = jnp.concatenate([every_cand, winners], axis=0)
        partial = lax.dot_general(
            rhs, emb[:, :, c * piece:(c + 1) * piece].reshape(points, piece), NT,
            preferred_element_type=jnp.float32,
        )
        sim[...] = partial if c == 0 else sim[...] + partial

    cover = jnp.max(sim[pl.ds(pl.multiple_of(mem * k1, k1), k1), :], axis=0, keepdims=True)
    lane = lax.broadcasted_iota(jnp.int32, (cands, 128), 1)
    gains = jnp.zeros((cands, 128), jnp.float32)
    for t in range(k2):
        acc = jnp.zeros((cands, 128), jnp.float32)
        for c in range(0, points, 128):
            acc = acc + jnp.maximum(sim[:cands, c:c + 128] - cover[:, c:c + 128], 0.0)
        gains = jnp.where(lane == t, jnp.sum(acc, axis=1, keepdims=True), gains)
        cover = jnp.maximum(cover, sim[cands + t:cands + t + 1, :])
    gsend[...] = gains.reshape(n_mem, k1, 128)
    gathers = [
        pltpu.make_async_remote_copy(
            src_ref=gsend.at[mem_peers[d]],
            dst_ref=gbuf.at[mem],
            send_sem=g_send.at[d - 1],
            recv_sem=g_recv.at[d - 1],
            device_id={"mem": mem_peers[d]},
            device_id_type=MESH,
        )
        for d in mem_far
    ]
    for copy in gathers:
        copy.start()
    gbuf[mem] = gsend[mem]

    for copy in shares:
        copy.wait_recv()
    total = zbuf[0].astype(jnp.float32)
    for g in range(1, n_grp):
        total = total + zbuf[g].astype(jnp.float32)
    zsum[...] = total.astype(jnp.bfloat16)
    finals = [
        pltpu.make_async_remote_copy(
            src_ref=zsum,
            dst_ref=fin.at[:, my_cols],
            send_sem=fin_send.at[d - 1],
            recv_sem=fin_recv.at[d - 1],
            device_id={"mem": mem_peers[d]},
            device_id_type=MESH,
        )
        for d in mem_near
    ]

    def send_final():
        for copy in finals:
            copy.start()
        fin[:, my_cols] = zsum[...]

    owner(send_final)

    if every:
        def piece_of(place):
            cols = pl.ds(pl.multiple_of(place * width, 128), width)
            return lax.dot_general(
                fin[:, cols], emb[:, :, cols].reshape(points, width), NT,
                preferred_element_type=jnp.float32,
            )

        best = piece_of(mem)
        for copy, d in zip(finals, mem_near):
            copy.wait_recv()
            best = best + piece_of(mem_peers[d])
    else:
        for d, copy in zip(mem_near, finals):
            pl.when(peer_of(mem, n_mem, d) < slices)(copy.wait_recv)
        best = lax.dot_general(
            fin[...], emb[...].reshape(points, depth), NT, preferred_element_type=jnp.float32
        )
    cover_ref[...] = jnp.max(best, axis=0, keepdims=True) * scale

    for copy in gathers:
        copy.wait_recv()
    total = jnp.sum(gbuf[...], axis=0) * (scale / points)
    gain_ref[...] = total[:, :k2]

    for copy in sum(bulks + relays, parts + shares + gathers):
        copy.wait_send()

    def sent_final():
        for copy in finals:
            copy.wait_send()

    owner(sent_final)


def per_device(n_grp, n_mem, embeddings, local_picks, second_picks, final_picks):
    points, depth = embeddings.shape
    k1 = local_picks.shape[1]
    k2 = second_picks.shape[1]
    k3 = final_picks.shape[0]
    cands = n_mem * k1
    slices = min(n_mem, depth // 128)
    width = depth // slices
    half = jnp.bfloat16
    dma = pltpu.SemaphoreType.DMA
    gain, cover = pl.pallas_call(
        functools.partial(kernel, n_grp, n_mem, slices),
        out_shape=(
            jax.ShapeDtypeStruct((k1, k2), jnp.float32),
            jax.ShapeDtypeStruct((1, points), jnp.float32),
        ),
        in_specs=[pl.BlockSpec(memory_space=pltpu.HBM)] * 4,
        out_specs=(pl.BlockSpec(memory_space=pltpu.VMEM),) * 2,
        scratch_shapes=[
            pltpu.VMEM((points // BLOCK, BLOCK, depth), half),
            pltpu.SMEM(local_picks.shape, jnp.int32),
            pltpu.SMEM(second_picks.shape, jnp.int32),
            pltpu.SMEM(final_picks.shape, jnp.int32),
            pltpu.VMEM((k1, depth), half),
            pltpu.VMEM((n_mem, k1, width), half),
            pltpu.VMEM((PIECES, n_mem, k1, depth // PIECES), half),
            pltpu.VMEM((n_grp, k3, width), half),
            pltpu.VMEM((k3, width), half),
            pltpu.VMEM((k3, depth), half),
            pltpu.VMEM((cands + k2, points), jnp.float32),
            pltpu.VMEM((n_mem, k1, 128), jnp.float32),
            pltpu.VMEM((n_mem, k1, 128), jnp.float32),
            dma((LOADS,)), dma((3,)),
            dma((n_mem - 1,)), dma((n_mem - 1,)),
            dma((PIECES, n_mem - 1)), dma((PIECES, n_mem - 1)),
            dma((n_grp - 1,)), dma((n_grp - 1,)),
            dma((n_mem - 1,)), dma((n_mem - 1,)),
            dma((n_mem - 1,)), dma((n_mem - 1,)),
        ],
        compiler_params=pltpu.CompilerParams(
            collective_id=0, has_side_effects=True, vmem_limit_bytes=48 * 1024 * 1024
        ),
    )(embeddings.reshape(points // BLOCK, BLOCK, depth),
      *[pltpu.with_memory_space_constraint(x, pltpu.HBM) for x in (local_picks, second_picks, final_picks)])
    return gain.T, cover.reshape(points)


def solution(mesh):
    n_grp, n_mem = mesh.shape["grp"], mesh.shape["mem"]
    return jax.shard_map(
        functools.partial(per_device, n_grp, n_mem),
        mesh=mesh,
        in_specs=(P(("grp", "mem"), None), P("grp", "mem"), P("grp", None), P()),
        out_specs=(P("grp", "mem"), P(("grp", "mem"))),
        check_vma=False,
    )
```

```python
import functools

import jax
import jax.numpy as jnp
from jax import lax
from jax.experimental import pallas as pl
from jax.experimental.pallas import tpu as pltpu
from jax.sharding import PartitionSpec as P

MESH = pl.DeviceIdType.MESH
NT = (((1,), (1,)), ((), ()))
LOADS = 8
BLOCK = 16
PIECES = 2


def kernel(
    n_grp, n_mem, slices,
    emb_hbm, local_hbm, second_hbm, final_hbm,
    gain_ref, cover_ref,
    emb, local, second, final, own, part, cand, zbuf, zsum, fin, sim, gsend, gbuf,
    load_sem, pick_sem, part_send, part_recv, cand_send, cand_recv,
    z_send, z_recv, fin_send, fin_recv, g_send, g_recv,
):
    grp = lax.axis_index("grp")
    mem = lax.axis_index("mem")
    tiles, block, depth = emb.shape
    points = tiles * block
    k1 = own.shape[0]
    k2 = second.shape[1]
    k3 = final.shape[0]
    cands = n_mem * k1
    width = depth // slices
    scale = float(depth) ** -0.5
    every = slices == n_mem

    def owner(body):
        if every:
            body()
        else:
            pl.when(mem < slices)(body)

    def peer_of(own_place, count, d):
        peer = own_place
        for bit in (1 << k for k in range(count.bit_length() - 1)):
            if d & bit:
                peer = peer + bit - 2 * bit * ((own_place // bit) % 2)
        return peer

    mem_far = range(n_mem - 1, 0, -1)
    mem_near = range(1, n_mem)
    across = range(2, n_mem, 2)
    grp_far = range(n_grp - 1, 0, -1)
    mem_peers = {d: peer_of(mem, n_mem, d) for d in mem_far}
    grp_peers = {d: peer_of(grp, n_grp, d) for d in grp_far}

    barrier = pltpu.get_barrier_semaphore()
    for d in mem_far:
        pl.semaphore_signal(barrier, inc=1, device_id={"mem": mem_peers[d]}, device_id_type=MESH)
    for d in grp_far:
        pl.semaphore_signal(barrier, inc=1, device_id={"grp": grp_peers[d]}, device_id_type=MESH)

    picks = [
        pltpu.make_async_copy(src, dst, pick_sem.at[i])
        for i, (src, dst) in enumerate(((local_hbm, local), (second_hbm, second), (final_hbm, final)))
    ]
    for copy in picks:
        copy.start()
    rows = tiles // LOADS
    loads = [
        pltpu.make_async_copy(
            emb_hbm.at[pl.ds(i * rows, rows)], emb.at[pl.ds(i * rows, rows)], load_sem.at[i]
        )
        for i in range(LOADS)
    ]
    for copy in loads:
        copy.start()
    for copy in picks:
        copy.wait()

    def one_hot(values, lanes):
        line = lax.broadcasted_iota(jnp.int32, (len(values), lanes), 0)
        spot = lax.broadcasted_iota(jnp.int32, (len(values), lanes), 1)
        wanted = jnp.zeros((len(values), lanes), jnp.int32)
        for r, value in enumerate(values):
            wanted = jnp.where(line == r, value, wanted)
        return jnp.where(spot == wanted, 1.0, 0.0).astype(jnp.bfloat16)

    shift = block.bit_length() - 1
    starts = [local[0, r] >> shift for r in range(k1)]
    choose = one_hot([r * block + (local[0, r] & (block - 1)) for r in range(k1)], k1 * block)
    seconds = one_hot([second[0, t] for t in range(k2)], cands)
    finals_of = one_hot([final[j] - grp * k2 for j in range(k3)], k2)
    table = jnp.dot(finals_of, seconds, preferred_element_type=jnp.float32).astype(jnp.bfloat16)

    for copy in loads:
        copy.wait()
    step = depth // 4
    for c in range(0, depth, step):
        blocks = jnp.concatenate(
            [emb[s, :, c:c + step] for s in starts], axis=0
        )
        own[:, c:c + step] = jnp.dot(
            choose, blocks, preferred_element_type=jnp.float32
        ).astype(jnp.bfloat16)
    pl.semaphore_wait(barrier, n_mem - 1 + n_grp - 1)

    def part_copy(d):
        peer = mem_peers[d]
        return pltpu.make_async_remote_copy(
            src_ref=own.at[:, pl.ds(pl.multiple_of(lax.rem(peer, slices) * width, 128), width)],
            dst_ref=part.at[mem],
            send_sem=part_send.at[d - 1],
            recv_sem=part_recv.at[d - 1],
            device_id={"mem": peer},
            device_id_type=MESH,
        )

    parts = [part_copy(d) for d in mem_near]
    for copy in parts:
        copy.start()
    chunks, piece = cand.shape[0], cand.shape[3]

    chunks, piece = cand.shape[0], cand.shape[3]

    def bulk_copy(c, d, source, at, to):
        return pltpu.make_async_remote_copy(
            src_ref=source,
            dst_ref=cand.at[c, at],
            send_sem=cand_send.at[c, d - 1],
            recv_sem=cand_recv.at[c, d - 1],
            device_id={"mem": to},
            device_id_type=MESH,
        )

    bulks, relays = [], []
    for c in range(chunks):
        mine = own.at[:, c * piece:(c + 1) * piece]
        bulks.append([bulk_copy(c, d, mine, mem, mem_peers[d]) for d in across])
        relays.append([bulk_copy(c, 1, mine, mem, mem_peers[1])] + [
            bulk_copy(c, d + 1, cand.at[c, mem_peers[d]], mem_peers[d], mem_peers[1])
            for d in across
        ])
    for chunk in bulks:
        for copy in chunk:
            copy.start()
    for chunk in relays:
        chunk[0].start()
    my_cols = pl.ds(pl.multiple_of(lax.rem(mem, slices) * width, 128), width)
    part[mem] = own[:, my_cols]
    for c in range(chunks):
        cand[c, mem] = own[:, c * piece:(c + 1) * piece]

    for copy in parts:
        copy.wait_recv()
    share = jnp.dot(
        table, part[...].reshape(cands, width), preferred_element_type=jnp.float32
    ).astype(jnp.bfloat16)
    zbuf[grp] = share
    shares = [
        pltpu.make_async_remote_copy(
            src_ref=zbuf.at[grp],
            dst_ref=zbuf.at[grp],
            send_sem=z_send.at[d - 1],
            recv_sem=z_recv.at[d - 1],
            device_id={"grp": grp_peers[d]},
            device_id_type=MESH,
        )
        for d in grp_far
    ]
    for copy in shares:
        copy.start()

    def relay(c):
        for copy, onward in zip(bulks[c], relays[c][1:]):
            copy.wait_recv()
            onward.start()

    relay(0)
    for c in range(chunks):
        if c + 1 < chunks:
            relay(c + 1)
        for copy in relays[c]:
            copy.wait_recv()
        every_cand = cand[c].reshape(cands, piece)
        winners = jnp.dot(
            seconds, every_cand, preferred_element_type=jnp.float32
        ).astype(jnp.bfloat16)
        rhs = jnp.concatenate([every_cand, winners], axis=0)
        partial = lax.dot_general(
            rhs, emb[:, :, c * piece:(c + 1) * piece].reshape(points, piece), NT,
            preferred_element_type=jnp.float32,
        )
        sim[...] = partial if c == 0 else sim[...] + partial

    cover = jnp.max(sim[pl.ds(pl.multiple_of(mem * k1, k1), k1), :], axis=0, keepdims=True)
    lane = lax.broadcasted_iota(jnp.int32, (cands, 128), 1)
    gains = jnp.zeros((cands, 128), jnp.float32)
    for t in range(k2 // 2):
        acc = jnp.zeros((cands, 128), jnp.float32)
        for c in range(0, points, 128):
            acc = acc + jnp.maximum(sim[:cands, c:c + 128] - cover[:, c:c + 128], 0.0)
        gains = jnp.where(lane == t, jnp.sum(acc, axis=1, keepdims=True), gains)
        cover = jnp.maximum(cover, sim[cands + t:cands + t + 1, :])
    for copy in shares:
        copy.wait_recv()
    total = zbuf[0].astype(jnp.float32)
    for g in range(1, n_grp):
        total = total + zbuf[g].astype(jnp.float32)
    zsum[...] = total.astype(jnp.bfloat16)
    finals = [
        pltpu.make_async_remote_copy(
            src_ref=zsum,
            dst_ref=fin.at[:, my_cols],
            send_sem=fin_send.at[d - 1],
            recv_sem=fin_recv.at[d - 1],
            device_id={"mem": mem_peers[d]},
            device_id_type=MESH,
        )
        for d in mem_near
    ]

    def send_final():
        for copy in finals:
            copy.start()
        fin[:, my_cols] = zsum[...]

    owner(send_final)

    for t in range(k2 // 2, k2):
        acc = jnp.zeros((cands, 128), jnp.float32)
        for c in range(0, points, 128):
            acc = acc + jnp.maximum(sim[:cands, c:c + 128] - cover[:, c:c + 128], 0.0)
        gains = jnp.where(lane == t, jnp.sum(acc, axis=1, keepdims=True), gains)
        cover = jnp.maximum(cover, sim[cands + t:cands + t + 1, :])
    gsend[...] = gains.reshape(n_mem, k1, 128)
    gathers = [
        pltpu.make_async_remote_copy(
            src_ref=gsend.at[mem_peers[d]],
            dst_ref=gbuf.at[mem],
            send_sem=g_send.at[d - 1],
            recv_sem=g_recv.at[d - 1],
            device_id={"mem": mem_peers[d]},
            device_id_type=MESH,
        )
        for d in mem_far
    ]
    for copy in gathers:
        copy.start()
    gbuf[mem] = gsend[mem]

    if every:
        def piece_of(place):
            cols = pl.ds(pl.multiple_of(place * width, 128), width)
            return lax.dot_general(
                fin[:, cols], emb[:, :, cols].reshape(points, width), NT,
                preferred_element_type=jnp.float32,
            )

        best = piece_of(mem)
        for copy, d in zip(finals, mem_near):
            copy.wait_recv()
            best = best + piece_of(mem_peers[d])
    else:
        for d, copy in zip(mem_near, finals):
            pl.when(peer_of(mem, n_mem, d) < slices)(copy.wait_recv)
        best = lax.dot_general(
            fin[...], emb[...].reshape(points, depth), NT, preferred_element_type=jnp.float32
        )
    cover_ref[...] = jnp.max(best, axis=0, keepdims=True) * scale

    for copy in gathers:
        copy.wait_recv()
    total = jnp.sum(gbuf[...], axis=0) * (scale / points)
    gain_ref[...] = total[:, :k2]

    for copy in sum(bulks + relays, parts + shares + gathers):
        copy.wait_send()

    def sent_final():
        for copy in finals:
            copy.wait_send()

    owner(sent_final)


def per_device(n_grp, n_mem, embeddings, local_picks, second_picks, final_picks):
    points, depth = embeddings.shape
    k1 = local_picks.shape[1]
    k2 = second_picks.shape[1]
    k3 = final_picks.shape[0]
    cands = n_mem * k1
    slices = min(n_mem, depth // 128)
    width = depth // slices
    half = jnp.bfloat16
    dma = pltpu.SemaphoreType.DMA
    gain, cover = pl.pallas_call(
        functools.partial(kernel, n_grp, n_mem, slices),
        out_shape=(
            jax.ShapeDtypeStruct((k1, k2), jnp.float32),
            jax.ShapeDtypeStruct((1, points), jnp.float32),
        ),
        in_specs=[pl.BlockSpec(memory_space=pltpu.HBM)] * 4,
        out_specs=(pl.BlockSpec(memory_space=pltpu.VMEM),) * 2,
        scratch_shapes=[
            pltpu.VMEM((points // BLOCK, BLOCK, depth), half),
            pltpu.SMEM(local_picks.shape, jnp.int32),
            pltpu.SMEM(second_picks.shape, jnp.int32),
            pltpu.SMEM(final_picks.shape, jnp.int32),
            pltpu.VMEM((k1, depth), half),
            pltpu.VMEM((n_mem, k1, width), half),
            pltpu.VMEM((PIECES, n_mem, k1, depth // PIECES), half),
            pltpu.VMEM((n_grp, k3, width), half),
            pltpu.VMEM((k3, width), half),
            pltpu.VMEM((k3, depth), half),
            pltpu.VMEM((cands + k2, points), jnp.float32),
            pltpu.VMEM((n_mem, k1, 128), jnp.float32),
            pltpu.VMEM((n_mem, k1, 128), jnp.float32),
            dma((LOADS,)), dma((3,)),
            dma((n_mem - 1,)), dma((n_mem - 1,)),
            dma((PIECES, n_mem - 1)), dma((PIECES, n_mem - 1)),
            dma((n_grp - 1,)), dma((n_grp - 1,)),
            dma((n_mem - 1,)), dma((n_mem - 1,)),
            dma((n_mem - 1,)), dma((n_mem - 1,)),
        ],
        compiler_params=pltpu.CompilerParams(
            collective_id=0, has_side_effects=True, vmem_limit_bytes=48 * 1024 * 1024
        ),
    )(embeddings.reshape(points // BLOCK, BLOCK, depth),
      *[pltpu.with_memory_space_constraint(x, pltpu.HBM) for x in (local_picks, second_picks, final_picks)])
    return gain.T, cover.reshape(points)


def solution(mesh):
    n_grp, n_mem = mesh.shape["grp"], mesh.shape["mem"]
    return jax.shard_map(
        functools.partial(per_device, n_grp, n_mem),
        mesh=mesh,
        in_specs=(P(("grp", "mem"), None), P("grp", "mem"), P("grp", None), P()),
        out_specs=(P("grp", "mem"), P(("grp", "mem"))),
        check_vma=False,
    )
```
